32 devices in a mesh: tm: 8 (over y, x, core), func: 4 (over z).
Axes of the slice: x: 2, y: 2, z: 4, core: 2. Of those that a mesh axis runs over, the one named last changes fastest.
Arguments:
- initial_values: float32 [512, 1024], P('func'), may hold values from -6 to 6
- sensor_columns: int32 [128], replicated, may hold values from 0 to 1023
- space_cells: int32 [4096], P('tm'), may hold values from 0 to 1023
- time_cells: int32 [4096], P('tm'), may hold values from 0 to 63
- trunk_head: float32 [2, 256], replicated, may hold values from -8 to 8
- trunk_layers: float32 [3, 256, 256], replicated, may hold values from -0.375 to 0.375
- trunk_shifts: float32 [4, 256], replicated, may hold values from -3 to 3
- branch_head: float32 [128, 256], replicated, may hold values from -0.5 to 0.5
- branch_layers: float32 [4, 256, 256], replicated, may hold values from -0.375 to 0.375
- branch_shifts: float32 [5, 256], replicated, may hold values from -3 to 3
Outputs:
- total_loss: float32 [1], replicated
- trunk_head_gradient: float32 [2, 256], replicated
- trunk_layers_gradient: float32 [3, 256, 256], replicated
- trunk_shifts_gradient: float32 [4, 256], replicated
- branch_head_gradient: float32 [128, 256], replicated
- branch_layers_gradient: float32 [4, 256, 256], replicated
- branch_shifts_gradient: float32 [5, 256], replicated
The draws below stay inside these ranges and needn't reach their ends.
All inputs are finite; a program needn't handle non-finite values.
Results may differ from the reference program's by a relative error of at most 0.00012.
Values sent between devices are 32-bit elements; how exact they have to be, the bound alone decides.
A program may use at most 128 MiB of HBM per device.

```python
import math
import jax
import jax.numpy as jnp
from jax import lax

PT_DEV = 512
SLAB_DEV = 4
WIDTH = 256
SENSORS = 128
TRUNK_DEPTH = 2
BRANCH_DEPTH = 3
GRID_X = 1024
GRID_T = 64
FUNCS = 512
POINTS = 4096
SLABS = 32
PT_SLAB = 128
N_TM = 8


def set_ends(entries, stream_key, least, largest):
    dims = entries.shape
    spot = [jax.random.randint(jax.random.fold_in(stream_key, axis), (), 0, dims[axis]) for axis in range(len(dims))]
    entries = entries.at[tuple(spot)].set(least)
    longest = dims.index(max(dims))
    spot[longest] = (spot[longest] + 1) % dims[longest]
    return entries.at[tuple(spot)].set(largest)


def level_of(stream_key, extent, split, low, largest):
    factor_of = 1.0
    for axis_at, shards_of in split:
        steps = jax.random.uniform(jax.random.fold_in(jax.random.fold_in(stream_key, 6), axis_at), (shards_of,), jnp.float32, low / len(split), largest / len(split))
        factor_of = factor_of * jnp.repeat(jnp.exp(steps), extent[axis_at] // shards_of).reshape((-1,) + (1,) * (len(extent) - 1 - axis_at))
    return factor_of


def centred(rng, dims, width, limit, split=(), held_as=jnp.bfloat16):
    loudness = level_of(rng, dims, split, -0.22, 0.18) if split else 1.0
    entries = jax.random.normal(rng, dims, jnp.float32) * width * loudness
    return jnp.minimum(jnp.maximum(entries, -limit), limit).astype(held_as)


def setup_inputs(seed: int = 0) -> dict:
    arg_keys = jax.random.split(jax.random.key(seed), 11)
    return {
        "initial_values": centred(arg_keys[0], (FUNCS, GRID_X), 1.0, 6.0, ((0, 4),), jnp.float32),
        "sensor_columns": set_ends(jax.random.randint(arg_keys[1], (SENSORS,), 0, GRID_X), jax.random.fold_in(arg_keys[1], 1), 0, GRID_X - 1).astype(jnp.int32),
        "space_cells": set_ends(jax.random.randint(arg_keys[2], (POINTS,), 0, GRID_X), jax.random.fold_in(arg_keys[2], 1), 0, GRID_X - 1).astype(jnp.int32),
        "time_cells": set_ends(jax.random.randint(arg_keys[3], (POINTS,), 0, GRID_T), jax.random.fold_in(arg_keys[3], 1), 0, GRID_T - 1).astype(jnp.int32),
        "trunk_head": centred(arg_keys[4], (2, WIDTH), 2.0, 8.0, (), jnp.float32),
        "trunk_layers": centred(arg_keys[5], (TRUNK_DEPTH + 1, WIDTH, WIDTH), WIDTH ** -0.5, 0.375, (), jnp.float32),
        "trunk_shifts": centred(arg_keys[6], (TRUNK_DEPTH + 2, WIDTH), 0.5, 3.0, (), jnp.float32),
        "branch_head": centred(arg_keys[7], (SENSORS, WIDTH), SENSORS ** -0.5, 0.5, (), jnp.float32),
        "branch_layers": centred(arg_keys[8], (BRANCH_DEPTH + 1, WIDTH, WIDTH), WIDTH ** -0.5, 0.375, (), jnp.float32),
        "branch_shifts": centred(arg_keys[9], (BRANCH_DEPTH + 2, WIDTH), 0.5, 3.0, (), jnp.float32),
    }


viscosity = 0.01 / math.pi
causal_rate = 3.0
epsilon = 1e-06
highest = lax.Precision.HIGHEST

def trunk_streams(params, space_points, time_points):
    head_rows, layers, shifts = params
    hidden_count = layers.shape[0] - 1
    breadth = layers.shape[2]
    values = jnp.tanh(space_points[:, None] * head_rows[0] + time_points[:, None] * head_rows[1] + shifts[0])
    slopes = 1.0 - values * values
    along_space = slopes * head_rows[0]
    along_time = slopes * head_rows[1]
    second_space = -2.0 * values * along_space * head_rows[0]
    for layer_index in range(hidden_count):
        stacked = jnp.stack([values, along_space, along_time, second_space], axis=1)
        inner_sum = jnp.dot(stacked.reshape(-1, breadth), layers[layer_index], precision=highest).reshape(stacked.shape)
        values = jnp.tanh(inner_sum[:, 0] + shifts[layer_index + 1])
        slopes = 1.0 - values * values
        along_space = slopes * inner_sum[:, 1]
        along_time = slopes * inner_sum[:, 2]
        second_space = slopes * inner_sum[:, 3] - 2.0 * values * along_space * inner_sum[:, 1]
    stacked = jnp.stack([values, along_space, along_time, second_space], axis=1)
    offset = jnp.concatenate([shifts[hidden_count + 1][None, :], jnp.zeros((3, breadth), jnp.float32)], axis=0)
    return jnp.dot(stacked.reshape(-1, breadth), layers[hidden_count], precision=highest).reshape(stacked.shape) + offset

def branch_features(params, sensors):
    head_rows, layers, shifts = params
    hidden_count = layers.shape[0] - 1
    hidden = jnp.tanh(jnp.dot(sensors, head_rows, precision=highest) + shifts[0])
    for layer_index in range(hidden_count):
        hidden = jnp.tanh(jnp.dot(hidden, layers[layer_index], precision=highest) + shifts[layer_index + 1])
    return jnp.dot(hidden, layers[hidden_count], precision=highest) + shifts[hidden_count + 1]

def residual_of(fields):
    return fields[:, 2] + fields[:, 0] * fields[:, 1] - viscosity * fields[:, 3]

def reference(initial_values, sensor_columns, space_cells, time_cells, trunk_head, trunk_layers, trunk_shifts, branch_head, branch_layers, branch_shifts):
    root_width = math.sqrt(WIDTH)
    norm_count = FUNCS * PT_SLAB
    sensors = jnp.take(initial_values, sensor_columns, axis=1)
    space_points = -1.0 + (2.0 * space_cells.astype(jnp.float32) + 1.0) / GRID_X
    slab_number = (jnp.arange(POINTS, dtype=jnp.int32) // PT_SLAB).astype(jnp.float32)
    time_points = (slab_number + (time_cells.astype(jnp.float32) + 0.5) / GRID_T) / SLABS
    space_blocks = space_points.reshape(N_TM, PT_DEV)
    time_blocks = time_points.reshape(N_TM, PT_DEV)
    trunk_params = (trunk_head, trunk_layers, trunk_shifts)
    branch_params = (branch_head, branch_layers, branch_shifts)

    def slab_sums(trunk_side, branch_side, space_block, time_block):
        features = branch_features(branch_side, sensors)
        streams = trunk_streams(trunk_side, space_block, time_block)
        fields = jnp.einsum('fk,psk->fsp', features, streams, precision=highest) / root_width
        residual = residual_of(fields)
        return lax.optimization_barrier(jnp.sum((residual * residual).reshape(FUNCS, SLAB_DEV, PT_SLAB), axis=(0, 2)))
    energy = lax.map(lambda blocks: slab_sums(trunk_params, branch_params, blocks[0], blocks[1]), (space_blocks, time_blocks)).reshape(SLABS) / norm_count
    before = jnp.cumsum(energy) - energy
    weights = jnp.exp(-causal_rate * before / (jnp.sum(energy) + epsilon))
    block_weights = weights.reshape(N_TM, SLAB_DEV)
    start_space = -1.0 + (2.0 * jnp.arange(GRID_X, dtype=jnp.int32).astype(jnp.float32) + 1.0) / GRID_X

    def start_loss(trunk_side, branch_side):
        features = branch_features(branch_side, sensors)
        start_basis = trunk_streams(trunk_side, start_space, jnp.zeros_like(start_space))[:, 0]
        start_error = jnp.dot(features, start_basis.T, precision=highest) / root_width - initial_values
        return jnp.mean(start_error * start_error)

    def block_loss(trunk_side, branch_side, space_block, time_block, slab_weights):
        return jnp.sum(slab_weights * slab_sums(trunk_side, branch_side, space_block, time_block)) / (norm_count * SLABS)
    start_value, start_gradients = jax.value_and_grad(start_loss, argnums=(0, 1))(trunk_params, branch_params)

    def accumulate(running, blocks):
        block_gradients = jax.grad(block_loss, argnums=(0, 1))(trunk_params, branch_params, blocks[0], blocks[1], blocks[2])
        return (jax.tree.map(jnp.add, running, block_gradients), None)
    gradients, unused = lax.scan(accumulate, start_gradients, (space_blocks, time_blocks, block_weights))
    total_loss = jnp.sum(weights * energy) / SLABS + start_value
    trunk_gradients, branch_gradients = gradients
    return (total_loss.reshape(1), trunk_gradients[0], trunk_gradients[1], trunk_gradients[2], branch_gradients[0], branch_gradients[1], branch_gradients[2])
```

```python
import functools
import math

import jax
import jax.numpy as jnp
from jax import lax
from jax.experimental import pallas as pl
from jax.experimental.pallas import tpu as pltpu
from jax.sharding import PartitionSpec as P

SLAB_DEV = 4
GRID_T = 64


viscosity = 0.01 / math.pi
causal_rate = 3.0
epsilon = 1e-06
vmem_limit = 60 * 1024 * 1024


MESH_ID = pl.DeviceIdType.MESH


def factors_of(size):
    found = []
    for base in (4, 2, 3, 5, 7):
        while size % base == 0 and size > 1:
            found.append(base)
            size //= base
    return found + ([size] if size > 1 else [])


def digit_phases(tm_size, func_size):
    phases, stride, left = [], 1, tm_size
    while left % 2 == 0 and left > 1:
        phases.append(("tm", stride, 2))
        stride, left = stride * 2, left // 2
    if left > 1:
        phases.append(("tm", stride, left))
    stride = 1
    for size in factors_of(func_size):
        phases.append(("func", stride, size))
        stride *= size
    return phases


def digits_here(tm_size, func_size):
    tm_rank, func_rank = lax.axis_index("tm"), lax.axis_index("func")
    found = []
    phases = digit_phases(tm_size, func_size)
    swap = len(phases) >= 3 and all(phases[k][0] == "tm" and phases[k][2] == 2 for k in range(3))
    for spot, (axis, stride, size) in enumerate(phases):
        rank = tm_rank if axis == "tm" else func_rank
        if swap and spot in (1, 2):
            core = lax.rem(tm_rank, 2)
            other = phases[3 - spot][1]
            stride = (1 - core) * stride + core * other
            digit = lax.rem(rank // phases[spot][1], 2) * (1 - core) + lax.rem(rank // other, 2) * core
        else:
            digit = lax.rem(rank // stride, size)

        def peer_of(step, axis=axis, stride=stride, size=size, digit=digit, rank=rank):
            target = lax.rem(digit + step, size)
            place = rank + (target - digit) * stride
            return target, ((place, func_rank) if axis == "tm" else (tm_rank, place))

        found.append((size, digit, peer_of))
    return found


def split(value):
    high = value.astype(jnp.bfloat16)
    return high, (value - high.astype(jnp.float32)).astype(jnp.bfloat16)


def product(left, right, left_dim, right_dim):
    def once(a, b):
        return lax.dot_general(
            a, b, (((left_dim,), (right_dim,)), ((), ())), preferred_element_type=jnp.float32
        )

    return once(left[0], right[0]) + (once(left[0], right[1]) + once(left[1], right[0]))


def column_sum(value):
    return jnp.sum(value, axis=0, keepdims=True)


def terms_kernel(
    factor,
    start_factor,
    initial_ref,
    target_ref,
    column_ref,
    place_ref,
    start_ref,
    head_ref,
    layers_ref,
    shifts_ref,
    branch_head_ref,
    branch_layers_ref,
    branch_shifts_ref,
    terms_ref,
    energy_ref,
    layer_high,
    layer_low,
    branch_high,
    branch_low,
    hidden_high,
    hidden_low,
    value_keep,
    inner_keep,
    branch_keep,
    branch_keep_high,
    branch_keep_low,
    sensor_high,
    sensor_low,
    feature_high,
    feature_low,
):
    depth, breadth = layers_ref.shape[0], layers_ref.shape[2]
    branch_depth = branch_layers_ref.shape[0]
    sensors_count = branch_head_ref.shape[0]
    slab_rows = place_ref.shape[0] // SLAB_DEV
    start_rows = start_ref.shape[0]
    inverse_root = 1.0 / math.sqrt(breadth)
    small = (depth + branch_depth) * breadth + sensors_count
    terms_ref[:, small:, :] = jnp.zeros((terms_ref.shape[0], terms_ref.shape[1] - small, breadth), jnp.float32)
    for layer in range(depth):
        layer_high[layer], layer_low[layer] = split(layers_ref[layer])
    for layer in range(branch_depth):
        branch_high[layer], branch_low[layer] = split(branch_layers_ref[layer])

    grid = initial_ref.shape[1]
    picks = lax.broadcasted_iota(jnp.int32, (grid, sensors_count), 0) == column_ref[...]
    picks = picks.astype(jnp.float32).astype(jnp.bfloat16)
    left = initial_ref[...]
    sensors = jnp.zeros((left.shape[0], sensors_count), jnp.float32)
    for piece in range(3):
        part = left.astype(jnp.bfloat16)
        left = left - part.astype(jnp.float32)
        sensors = sensors + jnp.dot(part, picks, preferred_element_type=jnp.float32)
    pair = split(sensors)
    sensor_high[...], sensor_low[...] = pair
    hidden = jnp.tanh(product(pair, split(branch_head_ref[...]), 1, 0) + branch_shifts_ref[0:1, :])
    for layer in range(branch_depth):
        pair = split(hidden)
        branch_keep[layer] = hidden
        branch_keep_high[layer], branch_keep_low[layer] = pair
        hidden = product(pair, (branch_high[layer], branch_low[layer]), 1, 0)
        hidden = hidden + branch_shifts_ref[layer + 1 : layer + 2, :]
        if layer < branch_depth - 1:
            hidden = jnp.tanh(hidden)
    feature_high[...], feature_low[...] = split(hidden)

    space_row, time_row = head_ref[0:1, :], head_ref[1:2, :]

    def trunk(places, rows, streams):
        total = rows * streams
        values = jnp.tanh(places[:, 0:1] * space_row + places[:, 1:2] * time_row + shifts_ref[0:1, :])
        parts = [values]
        if streams > 1:
            slopes = 1.0 - values * values
            along = slopes * space_row
            parts += [along, slopes * time_row, -2.0 * values * along * space_row]
        for layer in range(depth):
            value_keep[layer, :rows] = parts[0]
            for stream, part in enumerate(parts):
                high, low = split(part)
                hidden_high[layer, stream * rows : (stream + 1) * rows] = high
                hidden_low[layer, stream * rows : (stream + 1) * rows] = low
            inner = product(
                (hidden_high[layer, :total], hidden_low[layer, :total]),
                (layer_high[layer], layer_low[layer]),
                1,
                0,
            )
            parts = [inner[stream * rows : (stream + 1) * rows] for stream in range(streams)]
            parts[0] = parts[0] + shifts_ref[layer + 1 : layer + 2, :]
            if layer == depth - 1:
                break
            values = jnp.tanh(parts[0])
            if streams > 1:
                inner_keep[layer, :total] = inner
                slopes = 1.0 - values * values
                along = slopes * parts[1]
                parts = [
                    values,
                    along,
                    slopes * parts[2],
                    slopes * parts[3] - 2.0 * values * along * parts[1],
                ]
            else:
                parts = [values]
        for stream, part in enumerate(parts):
            high, low = split(part)
            hidden_high[depth, stream * rows : (stream + 1) * rows] = high
            hidden_low[depth, stream * rows : (stream + 1) * rows] = low

    def trunk_back(group, places, rows, streams, adjoint):
        total = rows * streams
        for layer in reversed(range(depth)):
            pair = split(adjoint)
            terms_ref[group, layer * breadth : (layer + 1) * breadth, :] = product(
                (hidden_high[layer, :total], hidden_low[layer, :total]), pair, 0, 0
            )
            terms_ref[group, small + 2 + layer + 1 : small + 2 + layer + 2, :] = column_sum(adjoint[:rows])
            outer = product(pair, (layer_high[layer], layer_low[layer]), 1, 1)
            values = value_keep[layer, :rows]
            slopes = 1.0 - values * values
            if streams > 1:
                over_value, over_space, over_time, over_second = (
                    outer[stream * rows : (stream + 1) * rows] for stream in range(streams)
                )
                if layer > 0:
                    space, time, second = (
                        inner_keep[layer - 1, stream * rows : (stream + 1) * rows]
                        for stream in range(1, streams)
                    )
                    bend = second - 2.0 * values * space * space
                else:
                    space, time = space_row, time_row
                    bend = -2.0 * values * space * space
                over_slope = space * over_space + time * over_time + bend * over_second
                over_value = (
                    over_value
                    - 2.0 * values * over_slope
                    - 2.0 * slopes * space * space * over_second
                )
                over_space = slopes * over_space - 4.0 * values * slopes * space * over_second
                adjoint = jnp.concatenate(
                    [slopes * over_value, over_space, slopes * over_time, slopes * over_second], axis=0
                )
            else:
                adjoint = slopes * outer
        over_value = adjoint[:rows]
        space_sum = places[:, 0:1] * over_value
        time_sum = places[:, 1:2] * over_value
        if streams > 1:
            space_sum = space_sum + adjoint[rows : 2 * rows]
            time_sum = time_sum + adjoint[2 * rows : 3 * rows]
        terms_ref[group, small : small + 1, :] = column_sum(space_sum)
        terms_ref[group, small + 1 : small + 2, :] = column_sum(time_sum)
        terms_ref[group, small + 2 : small + 3, :] = column_sum(over_value)

    def branch_back(group, adjoint):
        place = small + 2 + depth + 1
        for layer in reversed(range(branch_depth)):
            pair = split(adjoint)
            begin = (depth + layer) * breadth
            terms_ref[group, begin : begin + breadth, :] = product(
                (branch_keep_high[layer], branch_keep_low[layer]), pair, 0, 0
            )
            terms_ref[group, place + layer + 1 : place + layer + 2, :] = column_sum(adjoint)
            hidden = branch_keep[layer]
            adjoint = product(pair, (branch_high[layer], branch_low[layer]), 1, 1)
            adjoint = (1.0 - hidden * hidden) * adjoint
        terms_ref[group, small - sensors_count : small, :] = product(
            (sensor_high[...], sensor_low[...]), split(adjoint), 0, 0
        )
        terms_ref[group, place : place + 1, :] = column_sum(adjoint)

    def whole_sum(value):
        total = jnp.sum(jnp.sum(value, axis=0, keepdims=True), axis=1, keepdims=True)
        return jnp.broadcast_to(total, (1, 128))

    def slab(group, carry):
        rows = slab_rows
        places = place_ref[pl.ds(pl.multiple_of(group * rows, 8), rows), :]
        trunk(places, rows, 4)
        features = (feature_high[...], feature_low[...])
        basis = (hidden_high[depth], hidden_low[depth])
        fields = product(features, basis, 1, 1) * inverse_root
        field, field_x, field_t, field_xx = (
            fields[:, stream * rows : (stream + 1) * rows] for stream in range(4)
        )
        residual = field_t + field * field_x - viscosity * field_xx
        energy_ref[pl.ds(group, 1), :] = whole_sum(residual * residual)
        scaled = (factor * inverse_root) * residual
        pair = split(
            jnp.concatenate([scaled * field_x, scaled * field, scaled, -viscosity * scaled], axis=1)
        )
        branch_back(group, product(pair, basis, 1, 0))
        trunk_back(group, places, rows, 4, product(pair, features, 0, 0))
        return carry

    lax.fori_loop(0, SLAB_DEV, slab, 0)
    rows = start_rows
    places = start_ref[...]
    trunk(places, rows, 1)
    features = (feature_high[...], feature_low[...])
    basis = (hidden_high[depth, :rows], hidden_low[depth, :rows])
    error = product(features, basis, 1, 1) * inverse_root - target_ref[...]
    energy_ref[SLAB_DEV:, :] = jnp.broadcast_to(whole_sum(error * error), (8 - SLAB_DEV, 128))
    pair = split((start_factor * inverse_root) * error)
    branch_back(SLAB_DEV, product(pair, basis, 1, 0))
    trunk_back(SLAB_DEV, places, rows, 1, product(pair, features, 0, 0))


def reduce_kernel(
    tm_size, func_size, chunks, norm_count, start_count,
    terms_ref, own_ref, out_ref, loss_ref, every_ref, held_ref, *scratch,
):
    devices = tm_size * func_size
    phases = digits_here(tm_size, func_size)
    count = len(phases)
    landed, sums = scratch[:count], scratch[count : 2 * count]
    small_send, small_recv, send_sem, recv_sem, back_send, back_recv = scratch[2 * count :]
    tm_rank = lax.axis_index("tm")
    me = tm_rank * func_size + lax.axis_index("func")
    barrier = pltpu.get_barrier_semaphore()

    def device_of(other):
        return (other // func_size, lax.rem(other, func_size))

    def greet(step, carry):
        other = lax.rem(me + step, devices)
        pl.semaphore_signal(barrier, inc=1, device_id=device_of(other), device_id_type=MESH_ID)
        return carry

    lax.fori_loop(1, devices, greet, 0)
    every_ref[me] = own_ref[...]
    pl.semaphore_wait(barrier, devices - 1)

    def copy_of(step, slot, other):
        return pltpu.make_async_remote_copy(
            src_ref=own_ref,
            dst_ref=every_ref.at[slot],
            send_sem=small_send.at[step],
            recv_sem=small_recv.at[step],
            device_id=device_of(other),
            device_id_type=MESH_ID,
        )

    def send(step, carry):
        copy_of(step, me, lax.rem(me + step, devices)).start()
        return carry

    def receive(step, carry):
        source = lax.rem(me + devices - step, devices)
        copy = copy_of(step, source, source)
        copy.wait_send()
        copy.wait_recv()
        return carry

    lax.fori_loop(1, devices, send, 0)
    lax.fori_loop(1, devices, receive, 0)
    tiles = []
    for group in range(tm_size):
        tile = every_ref[group * func_size]
        for other in range(1, func_size):
            tile = tile + every_ref[group * func_size + other]
        tiles.append(tile)
    energies = [tile[row : row + 1] / norm_count for tile in tiles for row in range(SLAB_DEV)]
    before, running = [], jnp.zeros_like(energies[0])
    for energy in energies:
        before.append(running)
        running = running + energy
    weighted = jnp.zeros_like(running)
    own_weights = [weighted] * SLAB_DEV
    for spot, energy in enumerate(energies):
        weight = jnp.exp(-causal_rate * before[spot] / (running + epsilon))
        weighted = weighted + weight * energy
        row = spot % SLAB_DEV
        own_weights[row] = jnp.where(tm_rank == spot // SLAB_DEV, weight, own_weights[row])
    start_sum = sum(tile[SLAB_DEV : SLAB_DEV + 1] for tile in tiles)
    loss = weighted / (SLAB_DEV * tm_size) + start_sum / start_count
    loss_ref[...] = jnp.broadcast_to(loss, loss_ref.shape)
    columns = held_ref.shape[1]
    wide = [jnp.concatenate([weight] * (columns // 128), axis=1) for weight in own_weights]
    block = 64

    def combine(step, carry):
        here = pl.ds(pl.multiple_of(step * block, block), block)
        value = terms_ref[SLAB_DEV, here, :]
        for row in range(SLAB_DEV):
            value = value + wide[row] * terms_ref[row, here, :]
        held_ref[here, :] = value
        return carry

    lax.fori_loop(0, held_ref.shape[0] // block, combine, 0)

    copies_each = sum(size - 1 for size, digit, peer_of in phases)

    def total(chunk):
        rows = held_ref.shape[0] // chunks
        begin = chunk * rows
        held, base = held_ref, begin
        begins, sent = [], []
        number = chunk * copies_each
        for spot, (size, digit, peer_of) in enumerate(phases):
            begins.append((begin, rows))
            rows = rows // size
            copies = []
            for step in range(1, size):
                target, device = peer_of(step)
                copy = pltpu.make_async_remote_copy(
                    src_ref=held.at[pl.ds(pl.multiple_of(base + target * rows, 8), rows)],
                    dst_ref=landed[spot].at[chunk, step - 1],
                    send_sem=send_sem.at[number],
                    recv_sem=recv_sem.at[number],
                    device_id=device,
                    device_id_type=MESH_ID,
                )
                copy.start()
                copies.append(copy)
                number += 1
            yield
            value = held[pl.ds(pl.multiple_of(base + digit * rows, 8), rows), :]
            for step, copy in enumerate(copies):
                copy.wait_recv()
                value = value + landed[spot][chunk, step]
            sent.extend(copies)
            begin = begin + digit * rows
            if spot < count - 1:
                sums[spot][chunk] = value
                held, base = sums[spot].at[chunk], 0
            else:
                out_ref[pl.ds(pl.multiple_of(begin, 8), rows), :] = value
        number = chunk * copies_each
        for spot in reversed(range(count)):
            size, digit, peer_of = phases[spot]
            outer, outer_rows = begins[spot]
            width = outer_rows // size
            here = pl.ds(pl.multiple_of(outer + digit * width, 8), width)
            copies = []
            for step in range(1, size):
                copy = pltpu.make_async_remote_copy(
                    src_ref=out_ref.at[here],
                    dst_ref=out_ref.at[here],
                    send_sem=back_send.at[number],
                    recv_sem=back_recv.at[number],
                    device_id=peer_of(step)[1],
                    device_id_type=MESH_ID,
                )
                copy.start()
                sent.append(copy)
                source, device = peer_of(size - step)
                there = pl.ds(pl.multiple_of(outer + source * width, 8), width)
                copies.append(
                    pltpu.make_async_remote_copy(
                        src_ref=out_ref.at[there],
                        dst_ref=out_ref.at[there],
                        send_sem=back_send.at[number],
                        recv_sem=back_recv.at[number],
                        device_id=device,
                        device_id_type=MESH_ID,
                    )
                )
                number += 1
            yield
            for copy in copies:
                copy.wait_recv()
        for copy in sent:
            copy.wait_send()

    running_chunks = [total(chunk) for chunk in range(chunks)]
    while running_chunks:
        running_chunks = [each for each in running_chunks if next(each, True) is None]


def reduce_terms(terms, own, tm_size, func_size, norm_count, start_count):
    groups, total_rows, columns = terms.shape
    devices = tm_size * func_size
    chunks = 4
    while total_rows % (chunks * devices * 8):
        chunks //= 2
    rows = total_rows // chunks
    landed, sums, copies = [], [], 0
    for axis, stride, size in digit_phases(tm_size, func_size):
        rows //= size
        landed.append(pltpu.VMEM((chunks, size - 1, rows, columns), jnp.float32))
        sums.append(pltpu.VMEM((chunks, rows, columns), jnp.float32))
        copies += (size - 1) * chunks
    return pl.pallas_call(
        functools.partial(reduce_kernel, tm_size, func_size, chunks, norm_count, start_count),
        out_shape=(
            jax.ShapeDtypeStruct((total_rows, columns), jnp.float32),
            jax.ShapeDtypeStruct((8, 128), jnp.float32),
        ),
        in_specs=[pl.BlockSpec(memory_space=pltpu.VMEM)] * 2,
        out_specs=[pl.BlockSpec(memory_space=pltpu.VMEM)] * 2,
        scratch_shapes=[
            pltpu.VMEM((devices, 8, 128), jnp.float32),
            pltpu.VMEM((total_rows, columns), jnp.float32),
        ]
        + landed
        + sums
        + [pltpu.SemaphoreType.DMA((devices,))] * 2
        + [pltpu.SemaphoreType.DMA((copies,))] * 4,
        compiler_params=pltpu.CompilerParams(
            collective_id=0, has_side_effects=True, vmem_limit_bytes=vmem_limit
        ),
    )(terms, own)


def local(
    initial_values,
    sensor_columns,
    space_cells,
    time_cells,
    trunk_head,
    trunk_layers,
    trunk_shifts,
    branch_head,
    branch_layers,
    branch_shifts,
):
    time_groups = lax.axis_size("tm")
    func_groups = lax.axis_size("func")
    time_rank = lax.axis_index("tm")
    function_rows, grid_columns = initial_values.shape
    point_rows = space_cells.shape[0]
    breadth = trunk_head.shape[1]
    slab_rows = point_rows // SLAB_DEV
    slab_total = SLAB_DEV * time_groups
    norm_count = function_rows * func_groups * slab_rows
    start_count = function_rows * func_groups * grid_columns
    point_number = jnp.arange(point_rows, dtype=jnp.int32)
    slab_number = (time_rank * SLAB_DEV + point_number // slab_rows).astype(jnp.float32)
    space_points = -1.0 + (2.0 * space_cells.astype(jnp.float32) + 1.0) / grid_columns
    time_points = (slab_number + (time_cells.astype(jnp.float32) + 0.5) / GRID_T) / slab_total
    column_count = grid_columns // time_groups
    column_start = time_rank * column_count
    column_place = (column_start + jnp.arange(column_count, dtype=jnp.int32)).astype(jnp.float32)
    start_space = -1.0 + (2.0 * column_place + 1.0) / grid_columns
    targets = lax.dynamic_slice_in_dim(initial_values, column_start, column_count, 1)
    places = jnp.stack([space_points, time_points], axis=1)
    start_places = jnp.stack([start_space, jnp.zeros_like(start_space)], axis=1)
    depth, branch_depth = trunk_layers.shape[0], branch_layers.shape[0]
    sensors_count = branch_head.shape[0]
    shapes = (
        ("layers", (depth * breadth, breadth)),
        ("branch_layers", (branch_depth * breadth, breadth)),
        ("branch_head", branch_head.shape),
        ("head", trunk_head.shape),
        ("shifts", trunk_shifts.shape),
        ("branch_shifts", branch_shifts.shape),
    )
    used = sum(shape[0] for name, shape in shapes)
    unit = 8 * time_groups * func_groups
    total_rows = used + -used % unit
    stacked = 4 * slab_rows
    half, full = jnp.bfloat16, jnp.float32
    scratch = [
        ((depth, breadth, breadth), half),
        ((depth, breadth, breadth), half),
        ((branch_depth, breadth, breadth), half),
        ((branch_depth, breadth, breadth), half),
        ((depth + 1, stacked, breadth), half),
        ((depth + 1, stacked, breadth), half),
        ((depth, slab_rows, breadth), full),
        ((depth - 1, stacked, breadth), full),
        ((branch_depth, function_rows, breadth), full),
        ((branch_depth, function_rows, breadth), half),
        ((branch_depth, function_rows, breadth), half),
        ((function_rows, sensors_count), half),
        ((function_rows, sensors_count), half),
        ((function_rows, breadth), half),
        ((function_rows, breadth), half),
    ]
    terms, own = pl.pallas_call(
        functools.partial(terms_kernel, 2.0 / (norm_count * slab_total), 2.0 / start_count),
        out_shape=(
            jax.ShapeDtypeStruct((SLAB_DEV + 1, total_rows, breadth), jnp.float32),
            jax.ShapeDtypeStruct((8, 128), jnp.float32),
        ),
        in_specs=[pl.BlockSpec(memory_space=pltpu.VMEM)] * 11,
        out_specs=[pl.BlockSpec(memory_space=pltpu.VMEM)] * 2,
        scratch_shapes=[pltpu.VMEM(shape, kind) for shape, kind in scratch],
        compiler_params=pltpu.CompilerParams(vmem_limit_bytes=vmem_limit),
    )(
        initial_values,
        targets,
        sensor_columns.reshape(1, sensors_count),
        places,
        start_places,
        trunk_head,
        trunk_layers,
        trunk_shifts,
        branch_head,
        branch_layers,
        branch_shifts,
    )
    packed, loss = reduce_terms(terms, own, time_groups, func_groups, norm_count, start_count)
    summed, begin = {}, 0
    for name, shape in shapes:
        summed[name] = packed[begin : begin + shape[0]]
        begin += shape[0]
    return (
        loss[0, 0:1],
        summed["head"],
        summed["layers"].reshape(trunk_layers.shape),
        summed["shifts"],
        summed["branch_head"],
        summed["branch_layers"].reshape(branch_layers.shape),
        summed["branch_shifts"],
    )


def solution(mesh):
    in_specs = (P("func", None), P(), P("tm"), P("tm"), P(), P(), P(), P(), P(), P())
    out_specs = (P(), P(), P(), P(), P(), P(), P())
    return jax.shard_map(local, mesh=mesh, in_specs=in_specs, out_specs=out_specs, check_vma=False)
```

```python
import functools
import math

import jax
import jax.numpy as jnp
from jax import lax
from jax.experimental import pallas as pl
from jax.experimental.pallas import tpu as pltpu
from jax.sharding import PartitionSpec as P

SLAB_DEV = 4
GRID_T = 64


viscosity = 0.01 / math.pi
causal_rate = 3.0
epsilon = 1e-06
vmem_limit = 60 * 1024 * 1024


MESH_ID = pl.DeviceIdType.MESH


def factors_of(size):
    found = []
    for base in (4, 2, 3, 5, 7):
        while size % base == 0 and size > 1:
            found.append(base)
            size //= base
    return found + ([size] if size > 1 else [])


def digit_phases(tm_size, func_size):
    phases, stride, left = [], 1, tm_size
    while left % 2 == 0 and left > 1:
        phases.append(("tm", stride, 2))
        stride, left = stride * 2, left // 2
    if left > 1:
        phases.append(("tm", stride, left))
    stride = 1
    for size in factors_of(func_size):
        phases.append(("func", stride, size))
        stride *= size
    return phases


def digits_here(tm_size, func_size):
    tm_rank, func_rank = lax.axis_index("tm"), lax.axis_index("func")
    found = []
    phases = digit_phases(tm_size, func_size)
    swap = len(phases) >= 3 and all(phases[k][0] == "tm" and phases[k][2] == 2 for k in range(3))
    for spot, (axis, stride, size) in enumerate(phases):
        rank = tm_rank if axis == "tm" else func_rank
        if swap and spot in (1, 2):
            core = lax.rem(tm_rank, 2)
            other = phases[3 - spot][1]
            stride = (1 - core) * stride + core * other
            digit = lax.rem(rank // phases[spot][1], 2) * (1 - core) + lax.rem(rank // other, 2) * core
        else:
            digit = lax.rem(rank // stride, size)

        def peer_of(step, axis=axis, stride=stride, size=size, digit=digit, rank=rank):
            target = lax.rem(digit + step, size)
            place = rank + (target - digit) * stride
            return target, ((place, func_rank) if axis == "tm" else (tm_rank, place))

        found.append((size, digit, peer_of))
    return found


def split(value):
    high = value.astype(jnp.bfloat16)
    return high, (value - high.astype(jnp.float32)).astype(jnp.bfloat16)


def product(left, right, left_dim, right_dim):
    def once(a, b):
        return lax.dot_general(
            a, b, (((left_dim,), (right_dim,)), ((), ())), preferred_element_type=jnp.float32
        )

    return once(left[0], right[0]) + (once(left[0], right[1]) + once(left[1], right[0]))


def column_sum(value):
    return jnp.sum(value, axis=0, keepdims=True)


def terms_kernel(
    factor,
    start_factor,
    initial_ref,
    target_ref,
    column_ref,
    place_ref,
    start_ref,
    head_ref,
    layers_ref,
    shifts_ref,
    branch_head_ref,
    branch_layers_ref,
    branch_shifts_ref,
    terms_ref,
    energy_ref,
    layer_high,
    layer_low,
    branch_high,
    branch_low,
    hidden_high,
    hidden_low,
    value_keep,
    inner_keep,
    branch_keep,
    branch_keep_high,
    branch_keep_low,
    sensor_high,
    sensor_low,
    feature_high,
    feature_low,
):
    depth, breadth = layers_ref.shape[0], layers_ref.shape[2]
    branch_depth = branch_layers_ref.shape[0]
    sensors_count = branch_head_ref.shape[0]
    slab_rows = place_ref.shape[0] // SLAB_DEV
    start_rows = start_ref.shape[0]
    inverse_root = 1.0 / math.sqrt(breadth)
    small = (depth + branch_depth) * breadth + sensors_count
    terms_ref[:, small:, :] = jnp.zeros((terms_ref.shape[0], terms_ref.shape[1] - small, breadth), jnp.float32)
    for layer in range(depth):
        layer_high[layer], layer_low[layer] = split(layers_ref[layer])
    for layer in range(branch_depth):
        branch_high[layer], branch_low[layer] = split(branch_layers_ref[layer])

    grid = initial_ref.shape[1]
    picks = lax.broadcasted_iota(jnp.int32, (grid, sensors_count), 0) == column_ref[...]
    picks = picks.astype(jnp.float32).astype(jnp.bfloat16)
    left = initial_ref[...]
    sensors = jnp.zeros((left.shape[0], sensors_count), jnp.float32)
    for piece in range(3):
        part = left.astype(jnp.bfloat16)
        left = left - part.astype(jnp.float32)
        sensors = sensors + jnp.dot(part, picks, preferred_element_type=jnp.float32)
    pair = split(sensors)
    sensor_high[...], sensor_low[...] = pair
    hidden = jnp.tanh(product(pair, split(branch_head_ref[...]), 1, 0) + branch_shifts_ref[0:1, :])
    for layer in range(branch_depth):
        pair = split(hidden)
        branch_keep[layer] = hidden
        branch_keep_high[layer], branch_keep_low[layer] = pair
        hidden = product(pair, (branch_high[layer], branch_low[layer]), 1, 0)
        hidden = hidden + branch_shifts_ref[layer + 1 : layer + 2, :]
        if layer < branch_depth - 1:
            hidden = jnp.tanh(hidden)
    feature_high[...], feature_low[...] = split(hidden)

    space_row, time_row = head_ref[0:1, :], head_ref[1:2, :]

    def trunk(places, rows, streams):
        total = rows * streams
        values = jnp.tanh(places[:, 0:1] * space_row + places[:, 1:2] * time_row + shifts_ref[0:1, :])
        parts = [values]
        if streams > 1:
            slopes = 1.0 - values * values
            along = slopes * space_row
            parts += [along, slopes * time_row, -2.0 * values * along * space_row]
        for layer in range(depth):
            value_keep[layer, :rows] = parts[0]
            for stream, part in enumerate(parts):
                high, low = split(part)
                hidden_high[layer, stream * rows : (stream + 1) * rows] = high
                hidden_low[layer, stream * rows : (stream + 1) * rows] = low
            inner = product(
                (hidden_high[layer, :total], hidden_low[layer, :total]),
                (layer_high[layer], layer_low[layer]),
                1,
                0,
            )
            parts = [inner[stream * rows : (stream + 1) * rows] for stream in range(streams)]
            parts[0] = parts[0] + shifts_ref[layer + 1 : layer + 2, :]
            if layer == depth - 1:
                break
            values = jnp.tanh(parts[0])
            if streams > 1:
                inner_keep[layer, :total] = inner
                slopes = 1.0 - values * values
                along = slopes * parts[1]
                parts = [
                    values,
                    along,
                    slopes * parts[2],
                    slopes * parts[3] - 2.0 * values * along * parts[1],
                ]
            else:
                parts = [values]
        for stream, part in enumerate(parts):
            high, low = split(part)
            hidden_high[depth, stream * rows : (stream + 1) * rows] = high
            hidden_low[depth, stream * rows : (stream + 1) * rows] = low

    def trunk_back(group, places, rows, streams, adjoint):
        total = rows * streams
        for layer in reversed(range(depth)):
            pair = split(adjoint)
            terms_ref[group, layer * breadth : (layer + 1) * breadth, :] = product(
                (hidden_high[layer, :total], hidden_low[layer, :total]), pair, 0, 0
            )
            terms_ref[group, small + 2 + layer + 1 : small + 2 + layer + 2, :] = column_sum(adjoint[:rows])
            outer = product(pair, (layer_high[layer], layer_low[layer]), 1, 1)
            values = value_keep[layer, :rows]
            slopes = 1.0 - values * values
            if streams > 1:
                over_value, over_space, over_time, over_second = (
                    outer[stream * rows : (stream + 1) * rows] for stream in range(streams)
                )
                if layer > 0:
                    space, time, second = (
                        inner_keep[layer - 1, stream * rows : (stream + 1) * rows]
                        for stream in range(1, streams)
                    )
                    bend = second - 2.0 * values * space * space
                else:
                    space, time = space_row, time_row
                    bend = -2.0 * values * space * space
                over_slope = space * over_space + time * over_time + bend * over_second
                over_value = (
                    over_value
                    - 2.0 * values * over_slope
                    - 2.0 * slopes * space * space * over_second
                )
                over_space = slopes * over_space - 4.0 * values * slopes * space * over_second
                adjoint = jnp.concatenate(
                    [slopes * over_value, over_space, slopes * over_time, slopes * over_second], axis=0
                )
            else:
                adjoint = slopes * outer
        over_value = adjoint[:rows]
        space_sum = places[:, 0:1] * over_value
        time_sum = places[:, 1:2] * over_value
        if streams > 1:
            space_sum = space_sum + adjoint[rows : 2 * rows]
            time_sum = time_sum + adjoint[2 * rows : 3 * rows]
        terms_ref[group, small : small + 1, :] = column_sum(space_sum)
        terms_ref[group, small + 1 : small + 2, :] = column_sum(time_sum)
        terms_ref[group, small + 2 : small + 3, :] = column_sum(over_value)

    def branch_back(group, adjoint):
        place = small + 2 + depth + 1
        for layer in reversed(range(branch_depth)):
            pair = split(adjoint)
            begin = (depth + layer) * breadth
            terms_ref[group, begin : begin + breadth, :] = product(
                (branch_keep_high[layer], branch_keep_low[layer]), pair, 0, 0
            )
            terms_ref[group, place + layer + 1 : place + layer + 2, :] = column_sum(adjoint)
            hidden = branch_keep[layer]
            adjoint = product(pair, (branch_high[layer], branch_low[layer]), 1, 1)
            adjoint = (1.0 - hidden * hidden) * adjoint
        terms_ref[group, small - sensors_count : small, :] = product(
            (sensor_high[...], sensor_low[...]), split(adjoint), 0, 0
        )
        terms_ref[group, place : place + 1, :] = column_sum(adjoint)

    def whole_sum(value):
        total = jnp.sum(jnp.sum(value, axis=0, keepdims=True), axis=1, keepdims=True)
        return jnp.broadcast_to(total, (1, 128))

    def slab(group, carry):
        rows = slab_rows
        places = place_ref[pl.ds(pl.multiple_of(group * rows, 8), rows), :]
        trunk(places, rows, 4)
        features = (feature_high[...], feature_low[...])
        basis = (hidden_high[depth], hidden_low[depth])
        fields = product(features, basis, 1, 1) * inverse_root
        field, field_x, field_t, field_xx = (
            fields[:, stream * rows : (stream + 1) * rows] for stream in range(4)
        )
        residual = field_t + field * field_x - viscosity * field_xx
        energy_ref[pl.ds(group, 1), :] = whole_sum(residual * residual)
        scaled = (factor * inverse_root) * residual
        pair = split(
            jnp.concatenate([scaled * field_x, scaled * field, scaled, -viscosity * scaled], axis=1)
        )
        branch_back(group, product(pair, basis, 1, 0))
        trunk_back(group, places, rows, 4, product(pair, features, 0, 0))
        return carry

    lax.fori_loop(0, SLAB_DEV, slab, 0)
    rows = start_rows
    places = start_ref[...]
    trunk(places, rows, 1)
    features = (feature_high[...], feature_low[...])
    basis = (hidden_high[depth, :rows], hidden_low[depth, :rows])
    error = product(features, basis, 1, 1) * inverse_root - target_ref[...]
    energy_ref[SLAB_DEV:, :] = jnp.broadcast_to(whole_sum(error * error), (8 - SLAB_DEV, 128))
    pair = split((start_factor * inverse_root) * error)
    branch_back(SLAB_DEV, product(pair, basis, 1, 0))
    trunk_back(SLAB_DEV, places, rows, 1, product(pair, features, 0, 0))


def reduce_kernel(
    tm_size, func_size, chunks, norm_count, start_count,
    terms_ref, own_ref, out_ref, loss_ref, every_ref, held_ref, *scratch,
):
    devices = tm_size * func_size
    phases = digits_here(tm_size, func_size)
    count = len(phases)
    landed, sums = scratch[:count], scratch[count : 2 * count]
    small_send, small_recv, send_sem, recv_sem, back_send, back_recv = scratch[2 * count :]
    tm_rank = lax.axis_index("tm")
    me = tm_rank * func_size + lax.axis_index("func")
    barrier = pltpu.get_barrier_semaphore()

    def device_of(other):
        return (other // func_size, lax.rem(other, func_size))

    def greet(step, carry):
        other = lax.rem(me + step, devices)
        pl.semaphore_signal(barrier, inc=1, device_id=device_of(other), device_id_type=MESH_ID)
        return carry

    lax.fori_loop(1, devices, greet, 0)
    every_ref[me] = own_ref[...]
    pl.semaphore_wait(barrier, devices - 1)

    def copy_of(step, slot, other):
        return pltpu.make_async_remote_copy(
            src_ref=own_ref,
            dst_ref=every_ref.at[slot],
            send_sem=small_send.at[step],
            recv_sem=small_recv.at[step],
            device_id=device_of(other),
            device_id_type=MESH_ID,
        )

    def send(step, carry):
        copy_of(step, me, lax.rem(me + step, devices)).start()
        return carry

    def receive(step, carry):
        source = lax.rem(me + devices - step, devices)
        copy = copy_of(step, source, source)
        copy.wait_send()
        copy.wait_recv()
        return carry

    lax.fori_loop(1, devices, send, 0)
    lax.fori_loop(1, devices, receive, 0)
    tiles = []
    for group in range(tm_size):
        tile = every_ref[group * func_size]
        for other in range(1, func_size):
            tile = tile + every_ref[group * func_size + other]
        tiles.append(tile)
    energies = [tile[row : row + 1] / norm_count for tile in tiles for row in range(SLAB_DEV)]
    before, running = [], jnp.zeros_like(energies[0])
    for energy in energies:
        before.append(running)
        running = running + energy
    weighted = jnp.zeros_like(running)
    own_weights = [weighted] * SLAB_DEV
    for spot, energy in enumerate(energies):
        weight = jnp.exp(-causal_rate * before[spot] / (running + epsilon))
        weighted = weighted + weight * energy
        row = spot % SLAB_DEV
        own_weights[row] = jnp.where(tm_rank == spot // SLAB_DEV, weight, own_weights[row])
    start_sum = sum(tile[SLAB_DEV : SLAB_DEV + 1] for tile in tiles)
    loss = weighted / (SLAB_DEV * tm_size) + start_sum / start_count
    loss_ref[...] = jnp.broadcast_to(loss, loss_ref.shape)
    columns = held_ref.shape[1]
    wide = [jnp.concatenate([weight] * (columns // 128), axis=1) for weight in own_weights]
    block = 64

    def combine(step, carry):
        here = pl.ds(pl.multiple_of(step * block, block), block)
        value = terms_ref[SLAB_DEV, here, :]
        for row in range(SLAB_DEV):
            value = value + wide[row] * terms_ref[row, here, :]
        held_ref[here, :] = value
        return carry

    lax.fori_loop(0, held_ref.shape[0] // block, combine, 0)

    copies_each = sum(size - 1 for size, digit, peer_of in phases)

    def total(chunk):
        rows = held_ref.shape[0] // chunks
        begin = chunk * rows
        held, base = held_ref, begin
        begins, sent = [], []
        number = chunk * copies_each
        for spot, (size, digit, peer_of) in enumerate(phases):
            begins.append((begin, rows))
            rows = rows // size
            copies = []
            for step in range(1, size):
                target, device = peer_of(step)
                copy = pltpu.make_async_remote_copy(
                    src_ref=held.at[pl.ds(pl.multiple_of(base + target * rows, 8), rows)],
                    dst_ref=landed[spot].at[chunk, step - 1],
                    send_sem=send_sem.at[number],
                    recv_sem=recv_sem.at[number],
                    device_id=device,
                    device_id_type=MESH_ID,
                )
                copy.start()
                copies.append(copy)
                number += 1
            yield
            value = held[pl.ds(pl.multiple_of(base + digit * rows, 8), rows), :]
            for step, copy in enumerate(copies):
                copy.wait_recv()
                value = value + landed[spot][chunk, step]
            sent.extend(copies)
            begin = begin + digit * rows
            if spot < count - 1:
                sums[spot][chunk] = value
                held, base = sums[spot].at[chunk], 0
            else:
                out_ref[pl.ds(pl.multiple_of(begin, 8), rows), :] = value
        number = chunk * copies_each
        for spot in reversed(range(count)):
            size, digit, peer_of = phases[spot]
            outer, outer_rows = begins[spot]
            width = outer_rows // size
            here = pl.ds(pl.multiple_of(outer + digit * width, 8), width)
            copies = []
            for step in range(1, size):
                copy = pltpu.make_async_remote_copy(
                    src_ref=out_ref.at[here],
                    dst_ref=out_ref.at[here],
                    send_sem=back_send.at[number],
                    recv_sem=back_recv.at[number],
                    device_id=peer_of(step)[1],
                    device_id_type=MESH_ID,
                )
                copy.start()
                sent.append(copy)
                source, device = peer_of(size - step)
                there = pl.ds(pl.multiple_of(outer + source * width, 8), width)
                copies.append(
                    pltpu.make_async_remote_copy(
                        src_ref=out_ref.at[there],
                        dst_ref=out_ref.at[there],
                        send_sem=back_send.at[number],
                        recv_sem=back_recv.at[number],
                        device_id=device,
                        device_id_type=MESH_ID,
                    )
                )
                number += 1
            yield
            for copy in copies:
                copy.wait_recv()
        for copy in sent:
            copy.wait_send()

    running_chunks = [total(chunk) for chunk in range(chunks)]
    while running_chunks:
        running_chunks = [each for each in running_chunks if next(each, True) is None]


def reduce_terms(terms, own, tm_size, func_size, norm_count, start_count):
    groups, total_rows, columns = terms.shape
    devices = tm_size * func_size
    chunks = 4
    while total_rows % (chunks * devices * 8):
        chunks //= 2
    rows = total_rows // chunks
    landed, sums, copies = [], [], 0
    for axis, stride, size in digit_phases(tm_size, func_size):
        rows //= size
        landed.append(pltpu.VMEM((chunks, size - 1, rows, columns), jnp.float32))
        sums.append(pltpu.VMEM((chunks, rows, columns), jnp.float32))
        copies += (size - 1) * chunks
    return pl.pallas_call(
        functools.partial(reduce_kernel, tm_size, func_size, chunks, norm_count, start_count),
        out_shape=(
            jax.ShapeDtypeStruct((total_rows, columns), jnp.float32),
            jax.ShapeDtypeStruct((8, 128), jnp.float32),
        ),
        in_specs=[pl.BlockSpec(memory_space=pltpu.VMEM)] * 2,
        out_specs=[pl.BlockSpec(memory_space=pltpu.VMEM)] * 2,
        scratch_shapes=[
            pltpu.VMEM((devices, 8, 128), jnp.float32),
            pltpu.VMEM((total_rows, columns), jnp.float32),
        ]
        + landed
        + sums
        + [pltpu.SemaphoreType.DMA((devices,))] * 2
        + [pltpu.SemaphoreType.DMA((copies,))] * 4,
        compiler_params=pltpu.CompilerParams(
            collective_id=0, has_side_effects=True, vmem_limit_bytes=vmem_limit
        ),
    )(terms, own)


def unpack_kernel(packed_ref, *out_refs):
    begin = 0
    for out_ref in out_refs:
        rows = out_ref.shape[-2]
        if len(out_ref.shape) == 3:
            for layer in range(out_ref.shape[0]):
                out_ref[layer] = packed_ref[begin : begin + rows, :]
                begin += rows
        else:
            out_ref[...] = packed_ref[begin : begin + rows, :]
            begin += rows


def local(
    initial_values,
    sensor_columns,
    space_cells,
    time_cells,
    trunk_head,
    trunk_layers,
    trunk_shifts,
    branch_head,
    branch_layers,
    branch_shifts,
):
    time_groups = lax.axis_size("tm")
    func_groups = lax.axis_size("func")
    time_rank = lax.axis_index("tm")
    function_rows, grid_columns = initial_values.shape
    point_rows = space_cells.shape[0]
    breadth = trunk_head.shape[1]
    slab_rows = point_rows // SLAB_DEV
    slab_total = SLAB_DEV * time_groups
    norm_count = function_rows * func_groups * slab_rows
    start_count = function_rows * func_groups * grid_columns
    point_number = jnp.arange(point_rows, dtype=jnp.int32)
    slab_number = (time_rank * SLAB_DEV + point_number // slab_rows).astype(jnp.float32)
    space_points = -1.0 + (2.0 * space_cells.astype(jnp.float32) + 1.0) / grid_columns
    time_points = (slab_number + (time_cells.astype(jnp.float32) + 0.5) / GRID_T) / slab_total
    column_count = grid_columns // time_groups
    column_start = time_rank * column_count
    column_place = (column_start + jnp.arange(column_count, dtype=jnp.int32)).astype(jnp.float32)
    start_space = -1.0 + (2.0 * column_place + 1.0) / grid_columns
    targets = lax.dynamic_slice_in_dim(initial_values, column_start, column_count, 1)
    places = jnp.stack([space_points, time_points], axis=1)
    start_places = jnp.stack([start_space, jnp.zeros_like(start_space)], axis=1)
    depth, branch_depth = trunk_layers.shape[0], branch_layers.shape[0]
    sensors_count = branch_head.shape[0]
    shapes = (
        ("layers", (depth * breadth, breadth)),
        ("branch_layers", (branch_depth * breadth, breadth)),
        ("branch_head", branch_head.shape),
        ("head", trunk_head.shape),
        ("shifts", trunk_shifts.shape),
        ("branch_shifts", branch_shifts.shape),
    )
    used = sum(shape[0] for name, shape in shapes)
    unit = 8 * time_groups * func_groups
    total_rows = used + -used % unit
    stacked = 4 * slab_rows
    half, full = jnp.bfloat16, jnp.float32
    scratch = [
        ((depth, breadth, breadth), half),
        ((depth, breadth, breadth), half),
        ((branch_depth, breadth, breadth), half),
        ((branch_depth, breadth, breadth), half),
        ((depth + 1, stacked, breadth), half),
        ((depth + 1, stacked, breadth), half),
        ((depth, slab_rows, breadth), full),
        ((depth - 1, stacked, breadth), full),
        ((branch_depth, function_rows, breadth), full),
        ((branch_depth, function_rows, breadth), half),
        ((branch_depth, function_rows, breadth), half),
        ((function_rows, sensors_count), half),
        ((function_rows, sensors_count), half),
        ((function_rows, breadth), half),
        ((function_rows, breadth), half),
    ]
    terms, own = pl.pallas_call(
        functools.partial(terms_kernel, 2.0 / (norm_count * slab_total), 2.0 / start_count),
        out_shape=(
            jax.ShapeDtypeStruct((SLAB_DEV + 1, total_rows, breadth), jnp.float32),
            jax.ShapeDtypeStruct((8, 128), jnp.float32),
        ),
        in_specs=[pl.BlockSpec(memory_space=pltpu.VMEM)] * 11,
        out_specs=[pl.BlockSpec(memory_space=pltpu.VMEM)] * 2,
        scratch_shapes=[pltpu.VMEM(shape, kind) for shape, kind in scratch],
        compiler_params=pltpu.CompilerParams(vmem_limit_bytes=vmem_limit),
    )(
        initial_values,
        targets,
        sensor_columns.reshape(1, sensors_count),
        places,
        start_places,
        trunk_head,
        trunk_layers,
        trunk_shifts,
        branch_head,
        branch_layers,
        branch_shifts,
    )
    packed, loss = reduce_terms(terms, own, time_groups, func_groups, norm_count, start_count)
    parts = (trunk_layers, branch_layers, branch_head, trunk_head, trunk_shifts, branch_shifts)
    layers, branch, first, head, shifts, offsets = pl.pallas_call(
        unpack_kernel,
        out_shape=tuple(jax.ShapeDtypeStruct(part.shape, jnp.float32) for part in parts),
        in_specs=[pl.BlockSpec(memory_space=pltpu.VMEM)],
        out_specs=[pl.BlockSpec(memory_space=pltpu.VMEM)] * 6,
        compiler_params=pltpu.CompilerParams(vmem_limit_bytes=vmem_limit // 4),
    )(packed)
    return (loss[0, 0:1], head, layers, shifts, first, branch, offsets)


def solution(mesh):
    in_specs = (P("func", None), P(), P("tm"), P("tm"), P(), P(), P(), P(), P(), P())
    out_specs = (P(), P(), P(), P(), P(), P(), P())
    return jax.shard_map(local, mesh=mesh, in_specs=in_specs, out_specs=out_specs, check_vma=False)
```
